32 devices in a mesh: py: 2 (over x), px: 4 (over y, core), pz: 4 (over z).
Axes of the slice: x: 2, y: 2, z: 4, core: 2. Of those that a mesh axis runs over, the one named last changes fastest.
Arguments:
- initial_density: float32 [8, 256, 384, 128], P('py', 'px', 'pz'), may hold values from 0.2 to 1.8
- inverse_limit: float32 [8, 256, 384, 128], P('py', 'px', 'pz'), may hold values from 0.5 to 2
Outputs:
- temperature_end: float32 [8, 256, 384, 128], P('py', 'px', 'pz')
The draws below stay inside these ranges and needn't reach their ends.
All inputs are finite; a program needn't handle non-finite values.
Results may differ from the reference program's by a relative error of at most 0.00002.
Values sent between devices are 32-bit elements; how exact they have to be, the bound alone decides.
A program may use at most 384 MiB of HBM per device.

```python
import jax
import jax.numpy as jnp
from jax import lax

WIDTH_SECOND = 8
WIDTH_FIRST = 256
WIDTH_THIRD = 384
DEPTH_TOTAL = 128
STEPS = 3


def shard_levels(rng, shape, cuts, low, top_value):
    loudness = 1.0
    for position, shards_of in cuts:
        heights = jax.random.uniform(jax.random.fold_in(jax.random.fold_in(rng, 6), position), (shards_of,), jnp.float32, low / len(cuts), top_value / len(cuts))
        loudness = loudness * jnp.repeat(jnp.exp(heights), shape[position] // shards_of).reshape((-1,) + (1,) * (len(shape) - 1 - position))
    return loudness


def setup_inputs(seed: int = 0) -> dict:
    streams_of = jax.random.split(jax.random.key(seed), 3)
    return {
        "initial_density": jnp.clip(0.2 + 1.5999999 * jax.random.uniform(streams_of[0], (WIDTH_SECOND, WIDTH_FIRST, WIDTH_THIRD, DEPTH_TOTAL), jnp.float32) ** shard_levels(streams_of[0], (WIDTH_SECOND, WIDTH_FIRST, WIDTH_THIRD, DEPTH_TOTAL), ((0, 2), (1, 4), (2, 4)), -0.2, 0.2), 0.2, 1.8),
        "inverse_limit": jnp.clip(0.5 + 1.5 * jax.random.uniform(streams_of[1], (WIDTH_SECOND, WIDTH_FIRST, WIDTH_THIRD, DEPTH_TOTAL), jnp.float32) ** shard_levels(streams_of[1], (WIDTH_SECOND, WIDTH_FIRST, WIDTH_THIRD, DEPTH_TOTAL), ((0, 2), (1, 4), (2, 4)), -0.2, 0.2), 0.5, 2.0),
    }


def inner_cells(values, dims):
    for dim in dims:
        values = lax.slice_in_dim(values, 1, values.shape[dim] - 1, axis=dim)
    return values


def boundary_cells(values, dim, start, dims):
    remaining_parts = [other for other in dims if other != dim]
    values = inner_cells(values, remaining_parts)
    return lax.slice_in_dim(values, start, start + values.shape[dim] - 2, axis=dim)


def advance_population(haloed_population, inverse_limit):
    middle = inner_cells(haloed_population, (0, 1, 2))
    lower = [boundary_cells(haloed_population, dim, 0, (0, 1, 2)) for dim in (0, 1, 2)]
    upper = [boundary_cells(haloed_population, dim, 2, (0, 1, 2)) for dim in (0, 1, 2)]
    spread = lower[0] + upper[0] + lower[1] + upper[1] + lower[2] + upper[2] - 6.0 * middle
    return middle + 0.1 * spread + 0.2 * middle * (1.0 - middle * inverse_limit)


def reference(initial_density, inverse_limit):
    for step in range(STEPS):
        initial_density = advance_population(jnp.pad(initial_density, ((1, 1), (1, 1), (1, 1), (0, 0)), mode="constant"), inverse_limit)
    return initial_density
```

```python
import functools

import jax
import jax.numpy as jnp
from jax import lax
from jax.experimental import pallas as pl
from jax.experimental.pallas import tpu as pltpu
from jax.sharding import PartitionSpec as P

STEPS = 3
MESH = pl.DeviceIdType.MESH


def chunk_rows(rows):
    for parts in (8, 4, 2):
        if rows % parts == 0 and rows // parts >= 2:
            return rows // parts
    return rows


def kernel(sizes, x_ref, il_ref, out_ref, a_ref, il_v, hy, hx, hz, zs,
           load_sem, y_send, y_recv, x_send, x_recv, z_send, z_recv):
    ny, nx, nz = sizes
    planes, rows, depth, lanes = a_ref.shape
    size = chunk_rows(rows)
    chunks = rows // size
    axes = (("py", ny), ("px", nx), ("pz", nz))
    me = {axis: lax.axis_index(axis) for axis, _ in axes}
    has = {axis: (me[axis] > 0, me[axis] < n - 1) for axis, n in axes}

    def other(axis, side):
        return {axis: me[axis] + (2 * side - 1)}

    barrier = pltpu.get_barrier_semaphore()
    for axis, _ in axes:
        for side in (0, 1):
            @pl.when(has[axis][side])
            def _():
                pl.semaphore_signal(barrier, inc=1, device_id=other(axis, side), device_id_type=MESH)
    pl.semaphore_wait(barrier, sum(flag.astype(jnp.int32) for pair in has.values() for flag in pair))

    level = (a_ref, out_ref, a_ref, out_ref)

    def y_copy(step, side, c):
        span = pl.ds(c * size, size)
        source = x_ref if step == 0 else level[step]
        return pltpu.make_async_remote_copy(
            src_ref=source.at[(planes - 1) * side, span],
            dst_ref=hy.at[1 - side, step, span],
            send_sem=y_send.at[side, step, c],
            recv_sem=y_recv.at[1 - side, step, c],
            device_id=other("py", side), device_id_type=MESH)

    def y_landed(step, side, c):
        span = pl.ds(c * size, size)
        return pltpu.make_async_remote_copy(
            src_ref=x_ref.at[0, span],
            dst_ref=hy.at[side, step, span],
            send_sem=y_send.at[side, step, c],
            recv_sem=y_recv.at[side, step, c],
            device_id=other("py", side), device_id_type=MESH)

    def x_copy(step, side):
        return pltpu.make_async_remote_copy(
            src_ref=level[step].at[:, (rows - 1) * side],
            dst_ref=hx.at[1 - side, step],
            send_sem=x_send.at[side, step],
            recv_sem=x_recv.at[1 - side, step],
            device_id=other("px", side), device_id_type=MESH)

    def x_landed(step, side):
        return pltpu.make_async_remote_copy(
            src_ref=hx.at[side, step],
            dst_ref=hx.at[side, step],
            send_sem=x_send.at[side, step],
            recv_sem=x_recv.at[side, step],
            device_id=other("px", side), device_id_type=MESH)

    def z_copy(step, side):
        return pltpu.make_async_remote_copy(
            src_ref=zs.at[side, step],
            dst_ref=hz.at[1 - side, step],
            send_sem=z_send.at[side, step],
            recv_sem=z_recv.at[1 - side, step],
            device_id=other("pz", side), device_id_type=MESH)

    def z_landed(step, side):
        return pltpu.make_async_remote_copy(
            src_ref=hz.at[side, step],
            dst_ref=hz.at[side, step],
            send_sem=z_send.at[side, step],
            recv_sem=z_recv.at[side, step],
            device_id=other("pz", side), device_id_type=MESH)

    def start_y(step, c):
        for side in (0, 1):
            @pl.when(has["py"][side])
            def _():
                y_copy(step, side, c).start()

    def on_faces(make, axis, act):
        for side in (0, 1):
            @pl.when(has[axis][side])
            def _():
                act(make(side))

    @pl.loop(0, chunks)
    def _(c):
        start_y(0, c)

    loads = [
        pltpu.make_async_copy(x_ref.at[y], a_ref.at[y], load_sem.at[0, y]) for y in range(planes)
    ] + [
        pltpu.make_async_copy(il_ref.at[y], il_v.at[y], load_sem.at[1, y]) for y in range(planes)
    ]
    for load in loads:
        load.start()

    for side in (0, 1):
        @pl.when(jnp.logical_not(has["py"][side]))
        def _():
            for step in range(STEPS):
                @pl.loop(0, rows)
                def _(r):
                    hy[side, step, r] = jnp.zeros((depth, lanes), jnp.float32)

        @pl.when(jnp.logical_not(has["px"][side]))
        def _():
            for step in range(STEPS):
                for y in range(planes):
                    hx[side, step, y] = jnp.zeros((depth, lanes), jnp.float32)

        @pl.when(jnp.logical_not(has["pz"][side]))
        def _():
            for step in range(STEPS):
                for y in range(planes):
                    hz[side, step, y] = jnp.zeros((rows, lanes), jnp.float32)

    for load in loads:
        load.wait()

    @pl.loop(0, rows)
    def _(r):
        for y in range(planes):
            zs[0, 0, y, pl.ds(r, 1), :] = a_ref[y, r, 0:1, :]
            zs[1, 0, y, pl.ds(r, 1), :] = a_ref[y, r, depth - 1:depth, :]

    on_faces(functools.partial(x_copy, 0), "px", lambda copy: copy.start())
    on_faces(functools.partial(z_copy, 0), "pz", lambda copy: copy.start())

    place = lax.broadcasted_iota(jnp.int32, (depth, lanes), 0)

    def advance(step, r, below, above):
        old, new = level[step], level[step + 1]
        for y in range(planes):
            middle = old[y, r]
            first = hz[0, step, y, pl.ds(r, 1), :]
            last = hz[1, step, y, pl.ds(r, 1), :]
            total = below(y) + above(y)
            total += hy[0, step, r] if y == 0 else old[y - 1, r]
            total += hy[1, step, r] if y == planes - 1 else old[y + 1, r]
            total += jnp.where(place == 0, first, pltpu.roll(middle, 1, 0))
            total += jnp.where(place == depth - 1, last, pltpu.roll(middle, depth - 1, 0))
            value = 0.1 * total + middle * (0.6 - 0.2 * (middle * il_v[y, r]))
            new[y, r] = value
            if step < STEPS - 1:
                zs[0, step + 1, y, pl.ds(r, 1), :] = value[0:1]
                zs[1, step + 1, y, pl.ds(r, 1), :] = value[depth - 1:depth]

    for step in range(STEPS):
        old = level[step]

        on_faces(functools.partial(x_landed, step), "px", lambda copy: copy.wait_recv())
        on_faces(functools.partial(z_landed, step), "pz", lambda copy: copy.wait_recv())
        if step > 0:
            on_faces(functools.partial(x_copy, step - 1), "px", lambda copy: copy.wait_send())

        def arrive(c, step=step):
            for side in (0, 1):
                @pl.when(has["py"][side])
                def _():
                    y_landed(step, side, c).wait_recv()
                    if step > 0:
                        y_copy(step - 1, side, c).wait_send()

        def span(low, high, step=step, old=old):
            @pl.loop(low, high)
            def _(r):
                advance(step, r, lambda y: old[y, r - 1], lambda y: old[y, r + 1])

        arrive(0)
        advance(step, 0, lambda y: hx[0, step, y], lambda y: old[y, 1])
        span(1, size)

        @pl.loop(1, chunks - 1)
        def _(c):
            arrive(c)
            span(c * size, c * size + size)
            if step < STEPS - 1:
                start_y(step + 1, c - 1)

        arrive(chunks - 1)
        span(rows - size, rows - 1)
        advance(step, rows - 1, lambda y: old[y, rows - 2], lambda y: hx[1, step, y])
        if step < STEPS - 1:
            start_y(step + 1, chunks - 2)
            on_faces(functools.partial(x_copy, step + 1), "px", lambda copy: copy.start())
            on_faces(functools.partial(z_copy, step + 1), "pz", lambda copy: copy.start())
            start_y(step + 1, chunks - 1)

    on_faces(functools.partial(x_copy, STEPS - 1), "px", lambda copy: copy.wait_send())
    for step in range(STEPS):
        on_faces(functools.partial(z_copy, step), "pz", lambda copy: copy.wait_send())

    @pl.loop(0, chunks)
    def _(c):
        on_faces(lambda side: y_copy(STEPS - 1, side, c), "py", lambda copy: copy.wait_send())


def local(sizes, initial_density, inverse_limit):
    planes, rows, depth, lanes = initial_density.shape
    chunks = rows // chunk_rows(rows)
    dma = pltpu.SemaphoreType.DMA
    return pl.pallas_call(
        functools.partial(kernel, sizes),
        out_shape=pltpu.VMEM(initial_density.shape, jnp.float32),
        in_specs=[pl.BlockSpec(memory_space=pltpu.HBM)] * 2,
        out_specs=pl.BlockSpec(memory_space=pltpu.VMEM),
        scratch_shapes=[
            pltpu.VMEM((planes, rows, depth, lanes), jnp.float32),
            pltpu.VMEM((planes, rows, depth, lanes), jnp.float32),
            pltpu.VMEM((2, STEPS, rows, depth, lanes), jnp.float32),
            pltpu.VMEM((2, STEPS, planes, depth, lanes), jnp.float32),
            pltpu.VMEM((2, STEPS, planes, rows, lanes), jnp.float32),
            pltpu.VMEM((2, STEPS, planes, rows, lanes), jnp.float32),
            dma((2, planes)),
            dma((2, STEPS, chunks)), dma((2, STEPS, chunks)),
            dma((2, STEPS)), dma((2, STEPS)), dma((2, STEPS)), dma((2, STEPS)),
        ],
        compiler_params=pltpu.CompilerParams(
            collective_id=0, has_side_effects=True, vmem_limit_bytes=50 * 2**20),
        name="populate",
    )(initial_density, inverse_limit)


def solution(mesh):
    sizes = tuple(mesh.shape[axis] for axis in ("py", "px", "pz"))
    spec = P("py", "px", "pz", None)
    return jax.shard_map(functools.partial(local, sizes), mesh=mesh, in_specs=(spec, spec), out_specs=spec, check_vma=False)
```

```python
import functools

import jax
import jax.numpy as jnp
from jax import lax
from jax.experimental import pallas as pl
from jax.experimental.pallas import tpu as pltpu
from jax.sharding import PartitionSpec as P

STEPS = 3
PARTS = 4
MESH = pl.DeviceIdType.MESH


def chunk_rows(rows):
    for parts in (16, 8, 4, 2):
        if rows % parts == 0 and rows // parts >= 2:
            return rows // parts
    return rows


def kernel(sizes, x_ref, il_ref, out_ref, a_ref, il_v, hy, hx, hz, zs,
           load_sem, y_send, y_recv, x_send, x_recv, z_send, z_recv):
    ny, nx, nz = sizes
    planes, rows, depth, lanes = a_ref.shape
    size = chunk_rows(rows)
    chunks = rows // size
    axes = (("py", ny), ("px", nx), ("pz", nz))
    me = {axis: lax.axis_index(axis) for axis, _ in axes}
    has = {axis: (me[axis] > 0, me[axis] < n - 1) for axis, n in axes}

    def other(axis, side):
        return {axis: me[axis] + (2 * side - 1)}

    barrier = pltpu.get_barrier_semaphore()
    for axis, _ in axes:
        for side in (0, 1):
            @pl.when(has[axis][side])
            def _():
                pl.semaphore_signal(barrier, inc=1, device_id=other(axis, side), device_id_type=MESH)
    pl.semaphore_wait(barrier, sum(flag.astype(jnp.int32) for pair in has.values() for flag in pair))

    level = (a_ref, out_ref, a_ref, out_ref)

    def y_copy(step, side, c):
        span = pl.ds(c * size, size)
        source = x_ref if step == 0 else level[step]
        return pltpu.make_async_remote_copy(
            src_ref=source.at[(planes - 1) * side, span],
            dst_ref=hy.at[1 - side, step, span],
            send_sem=y_send.at[side, step, c],
            recv_sem=y_recv.at[1 - side, step, c],
            device_id=other("py", side), device_id_type=MESH)

    def y_landed(step, side, c):
        span = pl.ds(c * size, size)
        return pltpu.make_async_remote_copy(
            src_ref=x_ref.at[0, span],
            dst_ref=hy.at[side, step, span],
            send_sem=y_send.at[side, step, c],
            recv_sem=y_recv.at[side, step, c],
            device_id=other("py", side), device_id_type=MESH)

    def x_copy(step, side):
        return pltpu.make_async_remote_copy(
            src_ref=level[step].at[:, (rows - 1) * side],
            dst_ref=hx.at[1 - side, step],
            send_sem=x_send.at[side, step],
            recv_sem=x_recv.at[1 - side, step],
            device_id=other("px", side), device_id_type=MESH)

    def x_landed(step, side):
        return pltpu.make_async_remote_copy(
            src_ref=hx.at[side, step],
            dst_ref=hx.at[side, step],
            send_sem=x_send.at[side, step],
            recv_sem=x_recv.at[side, step],
            device_id=other("px", side), device_id_type=MESH)

    def z_copy(step, side):
        return pltpu.make_async_remote_copy(
            src_ref=zs.at[side, step],
            dst_ref=hz.at[1 - side, step],
            send_sem=z_send.at[side, step],
            recv_sem=z_recv.at[1 - side, step],
            device_id=other("pz", side), device_id_type=MESH)

    def z_landed(step, side):
        return pltpu.make_async_remote_copy(
            src_ref=hz.at[side, step],
            dst_ref=hz.at[side, step],
            send_sem=z_send.at[side, step],
            recv_sem=z_recv.at[side, step],
            device_id=other("pz", side), device_id_type=MESH)

    def start_y(step, c):
        for side in (0, 1):
            @pl.when(has["py"][side])
            def _():
                y_copy(step, side, c).start()

    def on_faces(make, axis, act):
        for side in (0, 1):
            @pl.when(has[axis][side])
            def _():
                act(make(side))

    @pl.loop(0, chunks)
    def _(c):
        start_y(0, c)

    loads = [
        pltpu.make_async_copy(x_ref.at[y], a_ref.at[y], load_sem.at[0, y]) for y in range(planes)
    ] + [
        pltpu.make_async_copy(il_ref.at[y], il_v.at[y], load_sem.at[1, y]) for y in range(planes)
    ]
    for load in loads:
        load.start()

    for side in (0, 1):
        @pl.when(jnp.logical_not(has["py"][side]))
        def _():
            for step in range(STEPS):
                @pl.loop(0, rows)
                def _(r):
                    hy[side, step, r] = jnp.zeros((depth, lanes), jnp.float32)

        @pl.when(jnp.logical_not(has["px"][side]))
        def _():
            for step in range(STEPS):
                for y in range(planes):
                    hx[side, step, y] = jnp.zeros((depth, lanes), jnp.float32)

        @pl.when(jnp.logical_not(has["pz"][side]))
        def _():
            for step in range(STEPS):
                for y in range(planes):
                    hz[side, step, y] = jnp.zeros((rows, lanes), jnp.float32)

    for load in loads:
        load.wait()

    @pl.loop(0, rows)
    def _(r):
        for y in range(planes):
            zs[0, 0, y, pl.ds(r, 1), :] = a_ref[y, r, 0:1, :]
            zs[1, 0, y, pl.ds(r, 1), :] = a_ref[y, r, depth - 1:depth, :]

    on_faces(functools.partial(x_copy, 0), "px", lambda copy: copy.start())
    on_faces(functools.partial(z_copy, 0), "pz", lambda copy: copy.start())

    place = lax.broadcasted_iota(jnp.int32, (depth, lanes), 0)

    def advance(step, r, below, above, ys=tuple(range(planes))):
        old, new = level[step], level[step + 1]
        for y in ys:
            middle = old[y, r]
            first = hz[0, step, y, pl.ds(r, 1), :]
            last = hz[1, step, y, pl.ds(r, 1), :]
            total = below(y) + above(y)
            total += hy[0, step, r] if y == 0 else old[y - 1, r]
            total += hy[1, step, r] if y == planes - 1 else old[y + 1, r]
            total += jnp.where(place == 0, first, pltpu.roll(middle, 1, 0))
            total += jnp.where(place == depth - 1, last, pltpu.roll(middle, depth - 1, 0))
            value = 0.1 * total + middle * (0.6 - 0.2 * (middle * il_v[y, r]))
            new[y, r] = value
            if step < STEPS - 1:
                zs[0, step + 1, y, pl.ds(r, 1), :] = value[0:1]
                zs[1, step + 1, y, pl.ds(r, 1), :] = value[depth - 1:depth]

    def span(step, low, high, ys):
        old = level[step]

        @pl.loop(low, high)
        def _(r):
            advance(step, r, lambda y: old[y, r - 1], lambda y: old[y, r + 1], ys)

    def head_rows(step, high, ys):
        old = level[step]
        advance(step, 0, lambda y: hx[0, step, y], lambda y: old[y, 1], ys)
        span(step, 1, high, ys)

    def tail_rows(step, low, ys):
        old = level[step]
        span(step, low, rows - 1, ys)
        advance(step, rows - 1, lambda y: old[y, rows - 2], lambda y: hx[1, step, y], ys)

    def arrive(step, side, c):
        y_landed(step, side, c).wait_recv()
        if step > 0:
            y_copy(step - 1, side, c).wait_send()

    every = tuple(range(planes))
    for step in range(STEPS):
        on_faces(functools.partial(x_landed, step), "px", lambda copy: copy.wait_recv())
        on_faces(functools.partial(z_landed, step), "pz", lambda copy: copy.wait_recv())
        if step > 0:
            on_faces(functools.partial(x_copy, step - 1), "px", lambda copy: copy.wait_send())

        if step == STEPS - 1:
            break

        def meet(c, step=step):
            for side in (0, 1):
                @pl.when(has["py"][side])
                def _():
                    arrive(step, side, c)

        meet(0)
        head_rows(step, size, every)

        @pl.loop(1, chunks - 1)
        def _(c):
            meet(c)
            span(step, c * size, c * size + size, every)
            start_y(step + 1, c - 1)

        meet(chunks - 1)
        tail_rows(step, rows - size, every)
        start_y(step + 1, chunks - 2)
        on_faces(functools.partial(x_copy, step + 1), "px", lambda copy: copy.start())
        on_faces(functools.partial(z_copy, step + 1), "pz", lambda copy: copy.start())
        start_y(step + 1, chunks - 1)

    step = STEPS - 1
    on_faces(functools.partial(x_copy, step), "px", lambda copy: copy.wait_send())
    for before in range(STEPS):
        on_faces(functools.partial(z_copy, before), "pz", lambda copy: copy.wait_send())

    def whole(ys):
        head_rows(step, size, ys)
        tail_rows(step, size, ys)

    if planes > 2:
        whole(every[1:-1])
    for side in (0, 1):
        @pl.when(jnp.logical_not(has["py"][side]))
        def _():
            whole((every[-side],))

    def outer(c, rows_of):
        for side in (0, 1):
            @pl.when(has["py"][side])
            def _():
                arrive(step, side, c)
                rows_of((every[-side],))

    outer(0, lambda ys: head_rows(step, size, ys))

    @pl.loop(1, chunks - 1)
    def _(c):
        outer(c, lambda ys: span(step, c * size, c * size + size, ys))

    outer(chunks - 1, lambda ys: tail_rows(step, rows - size, ys))

    @pl.loop(0, chunks)
    def _(c):
        on_faces(lambda side: y_copy(STEPS - 1, side, c), "py", lambda copy: copy.wait_send())


def deliver(parts, held_ref, out_ref, sems):
    planes, rows = out_ref.shape[:2]
    size = rows // parts
    copies = [
        pltpu.make_async_copy(
            held_ref.at[y, pl.ds(p * size, size)], out_ref.at[y, pl.ds(p * size, size)], sems.at[y, p])
        for y in range(planes) for p in range(parts)
    ]
    for copy in copies:
        copy.start()
    for copy in copies:
        copy.wait()


def local(sizes, initial_density, inverse_limit):
    planes, rows, depth, lanes = initial_density.shape
    chunks = rows // chunk_rows(rows)
    dma = pltpu.SemaphoreType.DMA
    held = pl.pallas_call(
        functools.partial(kernel, sizes),
        out_shape=pltpu.VMEM(initial_density.shape, jnp.float32),
        in_specs=[pl.BlockSpec(memory_space=pltpu.HBM)] * 2,
        out_specs=pl.BlockSpec(memory_space=pltpu.VMEM),
        scratch_shapes=[
            pltpu.VMEM((planes, rows, depth, lanes), jnp.float32),
            pltpu.VMEM((planes, rows, depth, lanes), jnp.float32),
            pltpu.VMEM((2, STEPS, rows, depth, lanes), jnp.float32),
            pltpu.VMEM((2, STEPS, planes, depth, lanes), jnp.float32),
            pltpu.VMEM((2, STEPS, planes, rows, lanes), jnp.float32),
            pltpu.VMEM((2, STEPS, planes, rows, lanes), jnp.float32),
            dma((2, planes)),
            dma((2, STEPS, chunks)), dma((2, STEPS, chunks)),
            dma((2, STEPS)), dma((2, STEPS)), dma((2, STEPS)), dma((2, STEPS)),
        ],
        compiler_params=pltpu.CompilerParams(
            collective_id=0, has_side_effects=True, vmem_limit_bytes=50 * 2**20),
        name="populate",
    )(initial_density, inverse_limit)
    parts = PARTS if rows % PARTS == 0 else 1
    return pl.pallas_call(
        functools.partial(deliver, parts),
        out_shape=jax.ShapeDtypeStruct(initial_density.shape, jnp.float32),
        in_specs=[pl.BlockSpec(memory_space=pltpu.VMEM)],
        out_specs=pl.BlockSpec(memory_space=pltpu.HBM),
        scratch_shapes=[dma((planes, parts))],
        compiler_params=pltpu.CompilerParams(vmem_limit_bytes=2**20),
        name="deliver",
    )(pltpu.with_memory_space_constraint(held, pltpu.VMEM))


def solution(mesh):
    sizes = tuple(mesh.shape[axis] for axis in ("py", "px", "pz"))
    spec = P("py", "px", "pz", None)
    return jax.shard_map(functools.partial(local, sizes), mesh=mesh, in_specs=(spec, spec), out_specs=spec, check_vma=False)
```
